32 devices in a mesh: dp: 8 (over z, x), col: 4 (over y, core).
Axes of the slice: x: 2, y: 2, z: 4, core: 2. Of those that a mesh axis runs over, the one named last changes fastest.
Arguments:
- tokens: bfloat16 [2048, 5120], P('dp', 'col'), may hold values from -72 to 72
- query_weight: bfloat16 [5120, 5120], P('dp', 'col'), may hold values from -0.078125 to 0.078125
- key_weight: bfloat16 [5120, 5120], P('dp', 'col'), may hold values from -0.078125 to 0.078125
- old_maps: bfloat16 [960, 8, 256, 256], P(None, 'dp', 'col'), may hold values from 9.9658966e-05 to 0.5
- pair_weight: bfloat16 [1000, 128], replicated, may hold values from -0.75 to 0.75
- pair_bias: float32 [128], replicated, may hold values from -1.5 to 1.5
- norm_gain: float32 [128], replicated, may hold values from 0.25 to 1.75
- norm_bias: float32 [128], replicated, may hold values from -1.5 to 1.5
- hidden_weight: bfloat16 [128, 512], replicated, may hold values from -0.5 to 0.5
- hidden_bias: float32 [512], replicated, may hold values from -1.5 to 1.5
- out_weight: bfloat16 [512, 128], replicated, may hold values from -0.25 to 0.25
- out_bias: float32 [128], replicated, may hold values from -1.5 to 1.5
- chain_starts: int32 [8, 8], P('dp'), may hold values from 0 to 244, as said below
- chain_lengths: int32 [8, 8], P('dp'), may hold values from 12 to 172
- chain_groups: int32 [8, 8], P('dp'), may hold values from 0 to 7, as said below
- tile_owner: int32 [8, 4, 8], P('dp', 'col'), may hold values from -1 to 7, as said below
Outputs:
- pair_tiles: bfloat16 [8, 8, 4, 2048, 128], P('dp', None, 'col')
The draws below stay inside these ranges and needn't reach their ends.
Inputs may be any that keep to these rules, and one draw needn't show every extreme that they name: `chain_starts`: in each bin the chains do not intersect, lie in increasing order and end exactly at token 256; between two chains at most 4 tokens belong to no chain. `chain_groups`: complex numbers start at 0 in each bin and never fall along the chains; only tokens of one complex attend to each other. `tile_owner`: A tile's owner is -1 exactly when the tile holds no pair of two tokens of one complex. Within one bin and key block, tiles have distinct owners; for each key block one owner receives a tile from every bin, so an owner receives at most 8 tiles of a key block.
All inputs are finite; a program needn't handle non-finite values.
Results may differ from the reference program's by a relative error of at most 0.012.
Values may be sent and summed in bfloat16 or wider, within the bound.
A program may use at most 192 MiB of HBM per device.

```python
import math
import jax
import jax.numpy as jnp
from jax import lax

D = 5120
HEADS = 40
HEAD = 128
CH_OLD = 960
PAIR = 128
PAIR_HID = 512
CHAINS_PER_BIN = 8
ROWT = 8
TOKENS_PER_BIN = 256
TOKENS = 2048
TILE = 2048
N_DP = 8
N_COL = 4


def chain_layout(key):
    folded = jax.random.fold_in(key, 11)
    random_seeds = jax.random.split(folded, 6)
    lower_limit = TOKENS_PER_BIN * 3 // 64
    upper_limit = TOKENS_PER_BIN * 7 // 64 + 1
    bin_rows = jnp.arange(N_DP, dtype=jnp.int32)[:, None]
    lead_cols = jnp.arange(CHAINS_PER_BIN - 1, dtype=jnp.int32)[None, :]
    leading_chain = jax.random.randint(random_seeds[0], (N_DP, CHAINS_PER_BIN - 1), lower_limit, upper_limit, dtype=jnp.int32)
    leading_chain = jnp.where(bin_rows == 1, lower_limit, leading_chain)
    leading_chain = jnp.where((bin_rows == 0) & (lead_cols == CHAINS_PER_BIN - 2), lower_limit, leading_chain).astype(jnp.int32)
    break_spacing = jax.random.randint(random_seeds[1], (N_DP, CHAINS_PER_BIN), 0, TOKENS_PER_BIN // 64 + 1, dtype=jnp.int32)
    break_spacing = jnp.where(bin_rows == 1, 0, break_spacing).astype(jnp.int32)
    closing = TOKENS_PER_BIN - jnp.sum(leading_chain, axis=1, keepdims=True) - jnp.sum(break_spacing, axis=1, keepdims=True)
    lengths = jnp.concatenate([leading_chain, closing], axis=1).astype(jnp.int32)
    lengths = jnp.where(bin_rows == 0, jnp.roll(lengths, 1, axis=1), lengths).astype(jnp.int32)
    starts = (jnp.cumsum(lengths + break_spacing, axis=1) - lengths).astype(jnp.int32)
    break_probability = jax.random.randint(random_seeds[2], (N_DP, 1), 0, 4, dtype=jnp.int32)
    break_probability = jnp.where(bin_rows == 0, 4, break_probability)
    chain_boundaries = (jax.random.randint(random_seeds[3], (N_DP, CHAINS_PER_BIN - 1), 0, 4, dtype=jnp.int32) < break_probability).astype(jnp.int32)
    groups = jnp.concatenate([jnp.zeros((N_DP, 1), jnp.int32), jnp.cumsum(chain_boundaries, axis=1).astype(jnp.int32)], axis=1)
    places = jnp.arange(TOKENS_PER_BIN, dtype=jnp.int32)
    member = (places[None, :, None] >= starts[:, None, :]) & (places[None, :, None] < (starts + lengths)[:, None, :])
    inside = jnp.any(member, axis=2)
    group_ids = jnp.sum(jnp.where(member, groups[:, None, :], 0), axis=2)
    same_group = inside[:, :, None] & inside[:, None, :] & (group_ids[:, :, None] == group_ids[:, None, :])
    live_tiles = jnp.any(same_group.reshape(N_DP, N_COL, TOKENS_PER_BIN // N_COL, ROWT, TOKENS_PER_BIN // ROWT), axis=(2, 4))
    tile_rank = jnp.cumsum(live_tiles.astype(jnp.int32), axis=2) - 1
    anchor = jax.random.randint(random_seeds[4], (N_COL,), 0, N_DP, dtype=jnp.int32)
    others = N_DP - 1
    order_keys = jax.random.randint(random_seeds[5], (N_DP, N_COL, others), 0, 4096, dtype=jnp.int32) * others + jnp.arange(others, dtype=jnp.int32)
    shuffled = jnp.argsort(order_keys, axis=2, stable=True).astype(jnp.int32)
    picked = jnp.take_along_axis(shuffled, jnp.clip(tile_rank - 1, 0, others - 1), axis=2)
    owners = jnp.where(tile_rank == 0, anchor[None, :, None], (anchor[None, :, None] + 1 + picked) % N_DP)
    owners = jnp.where(live_tiles, owners, -1).astype(jnp.int32)
    return (starts, lengths, groups, owners)


def draw_chain_starts(key, part):
    return chain_layout(key)[0]


def draw_chain_lengths(key, part):
    return chain_layout(key)[1]


def draw_chain_groups(key, part):
    return chain_layout(key)[2]


def draw_tile_owner(key, part):
    return chain_layout(key)[3]


def draw_tokens(key, part):
    random_seeds = jax.random.split(jax.random.fold_in(key, 3), 1)
    normals = jnp.clip(jax.random.normal(random_seeds[0], (TOKENS, D), jnp.float32), -6.0, 6.0)
    return normals.astype(jnp.bfloat16)


def block_scale(rng, dims, cuts, low, high):
    def one(position, shards_of):
        draws = jax.random.uniform(jax.random.fold_in(jax.random.fold_in(rng, 6), position), (shards_of,), jnp.float32, low / len(cuts), high / len(cuts))
        return jnp.repeat(jnp.exp(draws), dims[position] // shards_of).reshape((-1,) + (1,) * (len(dims) - position - 1))

    factor_of = one(*cuts[0])
    for cut in cuts[1:]:
        factor_of = factor_of * one(*cut)
    return factor_of


def scatter_about(key, shape, scale, limit, pieces=(), kind=jnp.bfloat16):
    drawn = jax.random.normal(key, shape, jnp.float32) * scale
    if len(pieces) > 0:
        drawn = block_scale(key, shape, pieces, -0.22, 0.18) * drawn
    return jnp.clip(drawn, min=-limit, max=limit).astype(kind)


def setup_inputs(seed: int = 0) -> dict:
    splits = jax.random.split(jax.random.key(seed), 17)
    tokens = draw_tokens(jax.random.fold_in(splits[16], 71), 0)
    query_weight = scatter_about(splits[1], (D, D), D ** -0.5, 0.078125, ((0, 8), (1, 4)))
    key_weight = scatter_about(splits[2], (D, D), D ** -0.5, 0.078125, ((0, 8), (1, 4)))
    old_maps = jnp.clip(jnp.exp(math.log(0.5) - 8.520609 * jax.random.uniform(splits[3], (CH_OLD, N_DP, TOKENS_PER_BIN, TOKENS_PER_BIN), jnp.float32) ** block_scale(splits[3], (CH_OLD, N_DP, TOKENS_PER_BIN, TOKENS_PER_BIN), ((1, 8), (2, 4)), -0.2, 0.2)), 9.965896606445312e-05, 0.5).astype(jnp.bfloat16)
    pair_weight = scatter_about(splits[4], (CH_OLD + HEADS, PAIR), 64 ** -0.5, 0.75)
    pair_bias = scatter_about(splits[5], (PAIR,), 0.3, 1.5, (), jnp.float32)
    norm_gain = jnp.clip(1.0 + 0.15 * jax.random.normal(splits[6], (PAIR,), jnp.float32), 0.25, 1.75)
    norm_bias = scatter_about(splits[7], (PAIR,), 0.3, 1.5, (), jnp.float32)
    hidden_weight = scatter_about(splits[8], (PAIR, PAIR_HID), PAIR ** -0.5, 0.5)
    hidden_bias = scatter_about(splits[9], (PAIR_HID,), 0.3, 1.5, (), jnp.float32)
    out_weight = scatter_about(splits[10], (PAIR_HID, PAIR), PAIR_HID ** -0.5, 0.25)
    out_bias = scatter_about(splits[11], (PAIR,), 0.3, 1.5, (), jnp.float32)
    chain_starts = draw_chain_starts(jax.random.fold_in(splits[16], 71), 0)
    chain_lengths = draw_chain_lengths(jax.random.fold_in(splits[16], 71), 0)
    chain_groups = draw_chain_groups(jax.random.fold_in(splits[16], 71), 0)
    tile_owner = draw_tile_owner(jax.random.fold_in(splits[16], 71), 0)
    return dict(tokens=tokens, query_weight=query_weight, key_weight=key_weight, old_maps=old_maps, pair_weight=pair_weight, pair_bias=pair_bias, norm_gain=norm_gain, norm_bias=norm_bias, hidden_weight=hidden_weight, hidden_bias=hidden_bias, out_weight=out_weight, out_bias=out_bias, chain_starts=chain_starts, chain_lengths=chain_lengths, chain_groups=chain_groups, tile_owner=tile_owner)


def chain_tokens(starts, lengths, groups, token_count):
    places = jnp.arange(token_count, dtype=jnp.int32)
    member = (places[:, None] >= starts[None, :]) & (places[:, None] < (starts + lengths)[None, :])
    inside = jnp.any(member, axis=1)
    group_ids = lax.optimization_barrier(jnp.sum(jnp.where(member, groups[None, :], 0), axis=1)).astype(jnp.int32)
    offset = lax.optimization_barrier(jnp.sum(jnp.where(member, places[:, None] - starts[None, :], 0), axis=1))
    return (inside, group_ids, offset.astype(jnp.float32))

def rotate(values, offset):
    half_width = values.shape[-1] // 2
    frequency = jnp.exp(jnp.arange(half_width).astype(jnp.float32) * (-2.0 * math.log(10000.0) / values.shape[-1]))
    angles = offset[:, None] * frequency[None, :]
    cosine = jnp.cos(angles)[:, None, :]
    sine_table = jnp.sin(angles)[:, None, :]
    former = values[..., :half_width]
    latter = values[..., half_width:]
    return jnp.concatenate([former * cosine - latter * sine_table, latter * cosine + former * sine_table], axis=-1)

def head_maps(queries, key_rows, allowed):
    scores = jnp.einsum('jhd,ihd->hji', key_rows.astype(jnp.float32), queries.astype(jnp.float32)) / math.sqrt(queries.shape[-1])
    masked = jnp.where(allowed[None], scores, -jnp.inf)
    largest = lax.optimization_barrier(jnp.max(masked, axis=1, keepdims=True))
    powers = jnp.exp(masked - largest)
    return (powers / lax.optimization_barrier(jnp.sum(powers, axis=1, keepdims=True))).astype(jnp.bfloat16)

def refine(pair_rows, valid, norm_gain, norm_bias, hidden_weight, hidden_bias, out_weight, out_bias):
    values = pair_rows.astype(jnp.float32)
    average = lax.optimization_barrier(jnp.mean(values, axis=-1, keepdims=True))
    centred = values - average
    spread = lax.optimization_barrier(jnp.mean(centred * centred, axis=-1, keepdims=True))
    normed = (centred * lax.rsqrt(spread + 1e-05) * norm_gain + norm_bias).astype(jnp.bfloat16)
    hidden = jnp.maximum(jnp.dot(normed, hidden_weight, preferred_element_type=jnp.float32) + hidden_bias, 0.0).astype(jnp.bfloat16)
    update = jnp.dot(hidden, out_weight, preferred_element_type=jnp.float32) + out_bias
    return (valid[:, None] * (values + update)).astype(jnp.bfloat16)

def reference(tokens, query_weight, key_weight, old_maps, pair_weight, pair_bias, norm_gain, norm_bias, hidden_weight, hidden_bias, out_weight, out_bias, chain_starts, chain_lengths, chain_groups, tile_owner):

    def one_bin(bin_index):
        bin_rows = lax.dynamic_slice_in_dim(tokens, (bin_index * TOKENS_PER_BIN).astype(jnp.int32), TOKENS_PER_BIN, 0)
        inside, group_ids, offset = chain_tokens(chain_starts[bin_index], chain_lengths[bin_index], chain_groups[bin_index], TOKENS_PER_BIN)
        queries = jnp.dot(bin_rows, query_weight, preferred_element_type=jnp.float32).reshape(TOKENS_PER_BIN, HEADS, HEAD)
        key_rows = jnp.dot(bin_rows, key_weight, preferred_element_type=jnp.float32).reshape(TOKENS_PER_BIN, HEADS, HEAD)
        queries = rotate(queries, offset).astype(jnp.bfloat16)
        key_rows = rotate(key_rows, offset).astype(jnp.bfloat16)
        same_group = inside[:, None] & inside[None, :] & (group_ids[:, None] == group_ids[None, :])
        allowed = same_group | jnp.eye(TOKENS_PER_BIN, dtype=bool)
        prob_maps = head_maps(queries, key_rows, allowed)
        earlier = lax.dynamic_index_in_dim(old_maps, bin_index, 1, keepdims=False).reshape(CH_OLD, TOKENS_PER_BIN * TOKENS_PER_BIN)
        pair_rows = jnp.dot(earlier.T, pair_weight[:CH_OLD], preferred_element_type=jnp.float32)
        pair_rows = pair_rows + jnp.dot(prob_maps.reshape(HEADS, TOKENS_PER_BIN * TOKENS_PER_BIN).T, pair_weight[CH_OLD:], preferred_element_type=jnp.float32)
        pair_rows = (pair_rows + pair_bias).astype(jnp.bfloat16)
        refined = refine(pair_rows, same_group.reshape(-1).astype(jnp.float32), norm_gain, norm_bias, hidden_weight, hidden_bias, out_weight, out_bias)
        blocks = refined.reshape(N_COL, TOKENS_PER_BIN // N_COL, ROWT, TOKENS_PER_BIN // ROWT, PAIR).astype(jnp.float32)
        owners = tile_owner[bin_index]
        select = (owners[None] == jnp.arange(N_DP, dtype=jnp.int32)[:, None, None]).astype(jnp.float32)
        placed = jnp.einsum('ocr,cjrip->ocjip', select, blocks)
        return placed.reshape(N_DP, N_COL, TILE, PAIR).astype(jnp.bfloat16)
    per_bin = lax.map(one_bin, jnp.arange(N_DP, dtype=jnp.int32))
    return jnp.swapaxes(per_bin, 0, 1)
```

```python
import math

import jax
import jax.numpy as jnp
from jax import lax
from jax.sharding import PartitionSpec as P

HEAD = 128


def chain_tokens(starts, lengths, groups, token_count):
    places = jnp.arange(token_count, dtype=jnp.int32)
    member = (places[:, None] >= starts[None, :]) & (places[:, None] < (starts + lengths)[None, :])
    inside = jnp.any(member, axis=1)
    group_ids = jnp.sum(jnp.where(member, groups[None, :], 0), axis=1)
    offset = jnp.sum(jnp.where(member, places[:, None] - starts[None, :], 0), axis=1)
    return (inside, group_ids, offset.astype(jnp.float32))


def rotate(values, offset):
    half_width = values.shape[-1] // 2
    frequency = jnp.exp(
        jnp.arange(half_width).astype(jnp.float32) * (-2.0 * math.log(10000.0) / values.shape[-1])
    )
    angles = offset[:, None] * frequency[None, :]
    cosine = jnp.cos(angles)[:, None, :]
    sine_table = jnp.sin(angles)[:, None, :]
    former = values[..., :half_width]
    latter = values[..., half_width:]
    return jnp.concatenate(
        [former * cosine - latter * sine_table, latter * cosine + former * sine_table], axis=-1
    )


def head_maps(queries, key_rows, allowed):
    scores = jnp.einsum(
        "jhd,ihd->hji", key_rows, queries, preferred_element_type=jnp.float32
    ) / math.sqrt(queries.shape[-1])
    masked = jnp.where(allowed[None], scores, -jnp.inf)
    largest = jnp.max(masked, axis=1, keepdims=True)
    powers = jnp.exp(masked - largest)
    return (powers / jnp.sum(powers, axis=1, keepdims=True)).astype(jnp.bfloat16)


def refine(
    pair_rows, valid, norm_gain, norm_bias, hidden_weight, hidden_bias, out_weight, out_bias
):
    values = pair_rows.astype(jnp.float32)
    average = jnp.mean(values, axis=-1, keepdims=True)
    centred = values - average
    spread = jnp.mean(centred * centred, axis=-1, keepdims=True)
    normed = (centred * lax.rsqrt(spread + 1e-05) * norm_gain + norm_bias).astype(jnp.bfloat16)
    hidden = jnp.maximum(
        jnp.dot(normed, hidden_weight, preferred_element_type=jnp.float32) + hidden_bias, 0.0
    ).astype(jnp.bfloat16)
    update = jnp.dot(hidden, out_weight, preferred_element_type=jnp.float32) + out_bias
    return (valid[:, None] * (values + update)).astype(jnp.bfloat16)


def body(
    tokens,
    query_weight,
    key_weight,
    old_maps,
    pair_weight,
    pair_bias,
    norm_gain,
    norm_bias,
    hidden_weight,
    hidden_bias,
    out_weight,
    out_bias,
    chain_starts,
    chain_lengths,
    chain_groups,
    tile_owner,
):
    column_count = lax.axis_size("col")
    row_count = lax.axis_size("dp")
    bin_tokens = tokens.shape[0]
    head_cols = query_weight.shape[1]
    by_rows = lax.all_to_all(tokens, "col", split_axis=0, concat_axis=1, tiled=True)
    share = by_rows.shape[0]
    depth = query_weight.shape[0]
    by_columns = lax.all_to_all(
        by_rows.reshape(share, row_count, depth), "dp", split_axis=1, concat_axis=1, tiled=True
    )
    columns = lax.all_gather(
        by_columns.reshape(share, row_count, depth).transpose(1, 0, 2), "col", axis=1, tiled=True
    ).reshape(row_count * bin_tokens, depth)

    def project(weight):
        partial = jnp.dot(columns, weight, preferred_element_type=jnp.float32)
        return lax.psum_scatter(
            partial.astype(jnp.bfloat16), "dp", scatter_dimension=0, tiled=True
        ).astype(jnp.float32)

    query_sum = project(query_weight)
    key_sum = project(key_weight)
    heads_here = head_cols // HEAD
    inside, group_ids, offset = chain_tokens(
        chain_starts[0], chain_lengths[0], chain_groups[0], bin_tokens
    )
    queries = rotate(query_sum.reshape(bin_tokens, heads_here, HEAD), offset).astype(jnp.bfloat16)
    key_rows = rotate(key_sum.reshape(bin_tokens, heads_here, HEAD), offset).astype(jnp.bfloat16)
    same_group = inside[:, None] & inside[None, :] & (group_ids[:, None] == group_ids[None, :])
    allowed = same_group | jnp.eye(bin_tokens, dtype=bool)
    prob_maps = head_maps(queries, key_rows, allowed)
    spread_maps = lax.all_to_all(prob_maps, "col", split_axis=1, concat_axis=0, tiled=True)
    block_width = bin_tokens // column_count
    start_key = lax.axis_index("col") * block_width
    key_group = lax.dynamic_slice_in_dim(same_group, start_key, block_width, 0)
    old_channels = old_maps.shape[0]
    earlier = old_maps.reshape(old_channels, -1)
    pair_rows = jnp.dot(earlier.T, pair_weight[:old_channels], preferred_element_type=jnp.float32)
    pair_rows = pair_rows + jnp.dot(
        spread_maps.reshape(spread_maps.shape[0], -1).T,
        pair_weight[old_channels:],
        preferred_element_type=jnp.float32,
    )
    pair_rows = (pair_rows + pair_bias).astype(jnp.bfloat16)
    owners = tile_owner[0, 0]
    row_tiles = owners.shape[0]
    tile_rows = bin_tokens // row_tiles
    pair_width = pair_rows.shape[1]
    select = (owners[None, :] == jnp.arange(row_count, dtype=jnp.int32)[:, None]).astype(
        jnp.bfloat16
    )
    refined = refine(
        pair_rows,
        key_group.reshape(-1).astype(jnp.float32),
        norm_gain,
        norm_bias,
        hidden_weight,
        hidden_bias,
        out_weight,
        out_bias,
    )
    outgoing = jnp.einsum(
        "dr,jrip->djip",
        select,
        refined.reshape(block_width, row_tiles, tile_rows, pair_width),
        preferred_element_type=jnp.float32,
    )
    outgoing = outgoing.astype(jnp.bfloat16).reshape(row_count, block_width * tile_rows, pair_width)
    arrived = lax.all_to_all(outgoing, "dp", split_axis=0, concat_axis=0, tiled=True)
    return arrived.reshape(1, row_count, 1, arrived.shape[1], pair_width)


def solution(mesh):
    in_specs = (
        P("dp", "col"),
        P("dp", "col"),
        P("dp", "col"),
        P(None, "dp", "col", None),
        P(),
        P(),
        P(),
        P(),
        P(),
        P(),
        P(),
        P(),
        P("dp", None),
        P("dp", None),
        P("dp", None),
        P("dp", "col", None),
    )
    out_specs = P("dp", None, "col", None, None)
    return jax.shard_map(body, mesh=mesh, in_specs=in_specs, out_specs=out_specs, check_vma=False)
```
